16 devices in a mesh: dp: 2 (over y, z), tp: 8 (over x, core).
Axes of the slice: x: 4, y: 2, z: 1, core: 2. Of those that a mesh axis runs over, the one named last changes fastest.
The devices are a block of a 4x4x8 slice.
Arguments:
- x: bfloat16 [48, 192, 5120], P('dp'), parts along dimension 0
- seq_lens: int32 [48], P('dp'), parts along dimension 0
- w_query: bfloat16 [5120, 5120], P(None, 'tp')
- w_key: bfloat16 [5120, 1024], P(None, 'tp')
- w_value: bfloat16 [5120, 1024], P(None, 'tp')
- w_out: bfloat16 [5120, 5120], P('tp')
- w_gate: bfloat16 [5120, 27648], P(None, 'tp')
- w_up: bfloat16 [5120, 27648], P(None, 'tp')
- w_down: bfloat16 [27648, 5120], P('tp')
- attn_gain: bfloat16 [5120], replicated
- mlp_gain: bfloat16 [5120], replicated
- k_cache: bfloat16 [48, 384, 8, 128], P('dp', None, 'tp'), parts along dimension 0
- v_cache: bfloat16 [48, 384, 8, 128], P('dp', None, 'tp'), parts along dimension 0
Outputs:
- output 1: bfloat16 [48, 192, 5120], P('dp'), parts along dimension 0
- output 2: bfloat16 [48, 384, 8, 128], P('dp', None, 'tp'), parts along dimension 0
- output 3: bfloat16 [48, 384, 8, 128], P('dp', None, 'tp'), parts along dimension 0
There are 2 independent parts. The reference program is written for one: setup_inputs(seed, part) draws one part's arguments, and reference() takes and returns one part's arrays. A program takes and returns all parts, laid end to end along the dimension named above; an argument that names none is the same for every part.
All inputs are finite; a program needn't handle non-finite values.
Results may differ from the reference program's by a relative error of at most 0.0113584.
Values are sent between devices in bfloat16 or wider.
A program may use at most 768 MiB of HBM per device.

```python
import jax
import jax.numpy as jnp
from jax import lax

D = 5120
HEADS = 40
KV_HEADS = 8
HEAD = 128
FF = 27648
BATCH = 24
SEQ = 192
CACHE_LEN = 384
TP = 8
EPS = 1e-5
ROPE_BASE = 10000.0


def setup_inputs(seed: int = 0, part: int = 0) -> dict:
    base_key = jax.random.key(seed)
    part_key = jax.random.fold_in(base_key, part)
    weight_keys = jax.random.split(base_key, 9)
    part_keys = jax.random.split(part_key, 5)
    qk_scale = 1.5 * D ** -0.5

    def normal_weight(rng_key, array_shape, factor):
        return (jax.random.normal(rng_key, array_shape, jnp.float32) * factor).astype(jnp.bfloat16)

    short_len = jax.random.randint(part_keys[1], (1,), SEQ // 2, (4 * SEQ) // 5 + 1)
    other_lens = jax.random.randint(part_keys[2], (BATCH - 1,), SEQ // 2, SEQ + 1)
    return {
        "x": normal_weight(part_keys[0], (BATCH, SEQ, D), 1.0),
        "seq_lens": jnp.concatenate([short_len, other_lens]).astype(jnp.int32),
        "w_query": normal_weight(weight_keys[0], (D, HEADS * HEAD), qk_scale),
        "w_key": normal_weight(weight_keys[1], (D, KV_HEADS * HEAD), qk_scale),
        "w_value": normal_weight(weight_keys[2], (D, KV_HEADS * HEAD), D ** -0.5),
        "w_out": normal_weight(weight_keys[3], (HEADS * HEAD, D), (HEADS * HEAD) ** -0.5),
        "w_gate": normal_weight(weight_keys[4], (D, FF), D ** -0.5),
        "w_up": normal_weight(weight_keys[5], (D, FF), D ** -0.5),
        "w_down": normal_weight(weight_keys[6], (FF, D), FF ** -0.5),
        "attn_gain": jax.random.uniform(weight_keys[7], (D,), jnp.float32, 0.5, 1.5).astype(jnp.bfloat16),
        "mlp_gain": jax.random.uniform(weight_keys[8], (D,), jnp.float32, 0.5, 1.5).astype(jnp.bfloat16),
        "k_cache": normal_weight(part_keys[3], (BATCH, CACHE_LEN, KV_HEADS, HEAD), 1.0),
        "v_cache": normal_weight(part_keys[4], (BATCH, CACHE_LEN, KV_HEADS, HEAD), 1.0),
    }


def rms_norm(rows, gain):
    rows32 = rows.astype(jnp.float32)
    inv_rms = lax.rsqrt(jnp.mean(rows32 * rows32, axis=-1, keepdims=True) + EPS)
    return (rows32 * inv_rms * gain.astype(jnp.float32)).astype(jnp.bfloat16)


def rotary(vecs, angles):
    half_dim = HEAD // 2
    pairs = vecs.reshape(vecs.shape[:-1] + (half_dim, 2))
    even_part = pairs[..., 0]
    odd_part = pairs[..., 1]
    cos_tab = jnp.cos(angles)[:, None, :]
    sin_tab = jnp.sin(angles)[:, None, :]
    turned = jnp.stack([even_part * cos_tab - odd_part * sin_tab, even_part * sin_tab + odd_part * cos_tab], axis=-1)
    return turned.reshape(vecs.shape)


def reference(x, seq_lens, w_query, w_key, w_value, w_out, w_gate, w_up, w_down, attn_gain, mlp_gain, k_cache, v_cache):
    group_size = HEADS // KV_HEADS
    heads_part = HEADS * HEAD // TP
    ff_part = FF // TP
    positions = jnp.arange(SEQ)
    inv_freq = ROPE_BASE ** (-jnp.arange(0, HEAD, 2).astype(jnp.float32) / HEAD)
    angles = positions.astype(jnp.float32)[:, None] * inv_freq[None, :]
    causal = positions[None, :] <= positions[:, None]

    def one_sequence(items):
        x_row, length = items
        normed = rms_norm(x_row, attn_gain)
        queries = rotary(jnp.dot(normed, w_query, preferred_element_type=jnp.float32).reshape(SEQ, HEADS, HEAD), angles).astype(jnp.bfloat16)
        keys = rotary(jnp.dot(normed, w_key, preferred_element_type=jnp.float32).reshape(SEQ, KV_HEADS, HEAD), angles).astype(jnp.bfloat16)
        values = jnp.dot(normed, w_value, preferred_element_type=jnp.float32).astype(jnp.bfloat16).reshape(SEQ, KV_HEADS, HEAD)
        valid = positions < length
        keys = jnp.where(valid[:, None, None], keys, jnp.zeros_like(keys))
        values = jnp.where(valid[:, None, None], values, jnp.zeros_like(values))
        allowed = causal & valid[None, :]

        def one_kv_head(blocks):
            q_block, k_block, v_block = blocks
            scores = jnp.einsum("qgh,sh->gqs", q_block.astype(jnp.float32), k_block.astype(jnp.float32)) * HEAD ** -0.5
            scores = jnp.where(allowed[None], scores, -jnp.inf)
            probs = jax.nn.softmax(scores, axis=-1).astype(jnp.bfloat16)
            mixed = jnp.einsum("gqs,sh->qgh", probs.astype(jnp.float32), v_block.astype(jnp.float32))
            return mixed.astype(jnp.bfloat16)

        q_grouped = jnp.transpose(queries.reshape(SEQ, KV_HEADS, group_size, HEAD), (1, 0, 2, 3))
        head_out = lax.map(one_kv_head, (q_grouped, jnp.transpose(keys, (1, 0, 2)), jnp.transpose(values, (1, 0, 2))))
        attn_rows = jnp.transpose(head_out, (1, 0, 2, 3)).reshape(SEQ, HEADS * HEAD)
        attn_sum = jnp.zeros((SEQ, D), jnp.float32)
        for index in range(TP):
            partial = jnp.dot(attn_rows[:, index * heads_part:(index + 1) * heads_part], w_out[index * heads_part:(index + 1) * heads_part], preferred_element_type=jnp.float32)
            attn_sum = attn_sum + partial.astype(jnp.bfloat16).astype(jnp.float32)
        hidden = (x_row.astype(jnp.float32) + attn_sum).astype(jnp.bfloat16)
        normed_mlp = rms_norm(hidden, mlp_gain)
        gate_pre = jnp.dot(normed_mlp, w_gate, preferred_element_type=jnp.float32)
        up_pre = jnp.dot(normed_mlp, w_up, preferred_element_type=jnp.float32)
        gated = (jax.nn.silu(gate_pre) * up_pre).astype(jnp.bfloat16)
        mlp_sum = jnp.zeros((SEQ, D), jnp.float32)
        for index in range(TP):
            partial = jnp.dot(gated[:, index * ff_part:(index + 1) * ff_part], w_down[index * ff_part:(index + 1) * ff_part], preferred_element_type=jnp.float32)
            mlp_sum = mlp_sum + partial.astype(jnp.bfloat16).astype(jnp.float32)
        out_row = (hidden.astype(jnp.float32) + mlp_sum).astype(jnp.bfloat16)
        return out_row, keys, values

    y, new_keys, new_values = lax.map(one_sequence, (x, seq_lens))
    k_cache_out = lax.dynamic_update_slice(k_cache, new_keys, (0, 0, 0, 0))
    v_cache_out = lax.dynamic_update_slice(v_cache, new_values, (0, 0, 0, 0))
    return y, k_cache_out, v_cache_out
```

```python
import jax
import jax.numpy as jnp
from jax import lax
from jax.experimental import pallas as pl
from jax.experimental.pallas import tpu as pltpu
from jax.sharding import PartitionSpec as P


EPS = 1e-5
ROPE_BASE = 10000.0
CHUNK_SEQS = (4, 4, 4, 4, 4, 4)


def rms_norm(rows, gain):
    rows32 = rows.astype(jnp.float32)
    inv_rms = lax.rsqrt(jnp.mean(rows32 * rows32, axis=-1, keepdims=True) + EPS)
    return (rows32 * inv_rms * gain.astype(jnp.float32)).astype(jnp.bfloat16)


def rotary(vecs):
    seq_len = vecs.shape[1]
    head_dim = vecs.shape[-1]
    half_dim = head_dim // 2
    inv_freq = ROPE_BASE ** (-jnp.arange(0, head_dim, 2).astype(jnp.float32) / head_dim)
    angles = jnp.arange(seq_len).astype(jnp.float32)[:, None] * inv_freq[None, :]
    table_shape = (1, seq_len) + (1,) * (vecs.ndim - 3) + (half_dim,)
    cos_tab = jnp.cos(angles).reshape(table_shape)
    sin_tab = jnp.sin(angles).reshape(table_shape)
    pairs = vecs.reshape(vecs.shape[:-1] + (half_dim, 2))
    even_part = pairs[..., 0]
    odd_part = pairs[..., 1]
    turned = jnp.stack([even_part * cos_tab - odd_part * sin_tab, even_part * sin_tab + odd_part * cos_tab], axis=-1)
    return turned.reshape(vecs.shape).astype(jnp.bfloat16)


def causal_attention(queries, keys, values, seq_lens):
    seq_len = queries.shape[1]
    head_dim = queries.shape[-1]
    scores = jnp.einsum("bqkgh,bskh->bkgqs", queries, keys, preferred_element_type=jnp.float32) * head_dim ** -0.5
    positions = jnp.arange(seq_len)
    allowed = (positions[None, None, :] <= positions[None, :, None]) & (positions[None, None, :] < seq_lens[:, None, None])
    scores = jnp.where(allowed[:, None, None], scores, -jnp.inf)
    probs = jax.nn.softmax(scores, axis=-1).astype(jnp.bfloat16)
    return jnp.einsum("bkgqs,bskh->bqkgh", probs, values, preferred_element_type=jnp.float32).astype(jnp.bfloat16)


def out_kernel(o_ref, w_ref, x_ref, h_ref):
    groups, _, depth = o_ref.shape
    total = jnp.zeros(h_ref.shape, jnp.float32)
    for group in range(groups):
        part = jnp.dot(o_ref[group], w_ref[pl.ds(group * depth, depth), :], preferred_element_type=jnp.float32)
        total = total + part.astype(jnp.bfloat16).astype(jnp.float32)
    h_ref[...] = (x_ref[...].astype(jnp.float32) + total).astype(jnp.bfloat16)


def out_project(o_rows, w_full, x_rows, tile):
    groups, rows, depth = o_rows.shape
    width = w_full.shape[1]
    return pl.pallas_call(
        out_kernel,
        grid=(width // tile,),
        in_specs=[
            pl.BlockSpec((groups, rows, depth), lambda n: (0, 0, 0)),
            pl.BlockSpec((groups * depth, tile), lambda n: (0, n)),
            pl.BlockSpec((rows, tile), lambda n: (0, n)),
        ],
        out_specs=pl.BlockSpec((rows, tile), lambda n: (0, n)),
        out_shape=jax.ShapeDtypeStruct((rows, width), jnp.bfloat16),
        compiler_params=pltpu.CompilerParams(vmem_limit_bytes=56 * 2**20),
        cost_estimate=pl.CostEstimate(flops=2 * rows * groups * depth * width, bytes_accessed=2 * groups * depth * width, transcendentals=0),
        name="out_project",
    )(o_rows, w_full, x_rows)


def solution(mesh):
    tp_size = mesh.shape["tp"]
    cores = 2
    chips = tp_size // cores

    def chip_perm(shift):
        return [(chip * cores + core, ((chip + shift) % chips) * cores + core) for chip in range(chips) for core in range(cores)]

    partner_perm = [(index, index ^ 1) for index in range(tp_size)]

    def places():
        index = lax.axis_index("tp")
        chip, core = lax.shift_right_logical(index, 1), index & 1
        return [core, 1 - core] + [(chip + shift) & (chips - 1) for shift in (0, 1, 2, chips - 1)]

    def reduce_rows(partial, resid_rows, where):
        rows = resid_rows.shape[0]
        width = partial.shape[-1]
        half = width // 2
        fence = lax.optimization_barrier

        def move(piece, perm):
            return lax.ppermute(piece, "tp", perm)

        def pick(array, axis, place):
            begin = [0] * array.ndim
            begin[axis] = place
            size = list(array.shape)
            size[axis] = 1
            return lax.squeeze(lax.dynamic_slice(array, begin, size, allow_negative_indices=False), (axis,))

        partial, where = fence((partial, where))
        blocks = partial.reshape(chips, cores, rows, width)
        keep, give = fence((pick(blocks, 1, where[0]), pick(blocks, 1, where[1])))
        got = move(give, partner_perm)
        low, high = slice(0, half), slice(half, width)

        def both(place, columns):
            return pick(keep, 0, place)[:, columns].astype(jnp.float32) + pick(got, 0, place)[:, columns].astype(jnp.float32)

        keep, got, where = fence((keep, got, where))
        pieces = fence((both(where[4], low), both(where[4], high), both(where[3], high), both(where[5], low)))
        far_low = move(pieces[0], chip_perm(1))
        far_high = move(pieces[1], chip_perm(-1))
        near_high = move(pieces[2], chip_perm(1))
        near_low = move(pieces[3], chip_perm(-1))
        keep, got, where, far_low, far_high = fence((keep, got, where, far_low, far_high))
        pieces = fence((both(where[3], low) + far_low, both(where[5], high) + far_high))
        run_low = move(pieces[0], chip_perm(1))
        run_high = move(pieces[1], chip_perm(-1))
        keep, got, where, near_low, near_high, run_low, run_high = fence((keep, got, where, near_low, near_high, run_low, run_high))
        sum_low = both(where[2], low) + near_low + run_low
        sum_high = both(where[2], high) + near_high + run_high
        summed = jnp.concatenate([sum_low, sum_high], axis=1)
        return fence((resid_rows.astype(jnp.float32) + summed).astype(jnp.bfloat16))

    def layer_shard(x, seq_lens, w_query, w_key, w_value, w_out, w_gate, w_up, w_down, attn_gain, mlp_gain, k_cache, v_cache):
        batch_size, seq_len, model_width = x.shape
        head_dim = k_cache.shape[3]
        kv_local = k_cache.shape[2]
        group_size = w_query.shape[1] // (head_dim * kv_local)
        all_rows = batch_size * seq_len
        chunk_rows = [seqs * seq_len for seqs in CHUNK_SEQS]
        starts = [sum(chunk_rows[:chunk]) for chunk in range(len(chunk_rows))]
        tp_index = lax.axis_index("tp")
        w_out_full = lax.all_gather(w_out, "tp", axis=0, tiled=True)
        normed = rms_norm(x, attn_gain)
        queries = rotary(jnp.einsum("bsd,dk->bsk", normed, w_query, preferred_element_type=jnp.float32).reshape(batch_size, seq_len, kv_local, group_size, head_dim))
        keys = rotary(jnp.einsum("bsd,dk->bsk", normed, w_key, preferred_element_type=jnp.float32).reshape(batch_size, seq_len, kv_local, head_dim))
        values = jnp.einsum("bsd,dk->bsk", normed, w_value, preferred_element_type=jnp.float32).astype(jnp.bfloat16).reshape(batch_size, seq_len, kv_local, head_dim)
        valid = (jnp.arange(seq_len)[None, :] < seq_lens[:, None])[:, :, None, None]
        keys = jnp.where(valid, keys, jnp.zeros_like(keys))
        values = jnp.where(valid, values, jnp.zeros_like(values))
        k_cache_out = lax.dynamic_update_slice(k_cache, keys, (0, 0, 0, 0))
        v_cache_out = lax.dynamic_update_slice(v_cache, values, (0, 0, 0, 0))
        attn_rows = causal_attention(queries, keys, values, seq_lens).reshape(all_rows, -1)

        def by_owner(array):
            pieces = [array[start:start + size].reshape(tp_size, size // tp_size, array.shape[1]) for start, size in zip(starts, chunk_rows)]
            return jnp.concatenate(pieces, axis=1)

        o_rows = lax.all_to_all(by_owner(attn_rows), "tp", 0, 0, tiled=True)
        x_rows = jnp.concatenate([lax.dynamic_slice_in_dim(x.reshape(all_rows, model_width), start + tp_index * (size // tp_size), size // tp_size, axis=0) for start, size in zip(starts, chunk_rows)], axis=0)
        hidden_rows = out_project(o_rows, w_out_full, x_rows, 512)
        normed_rows = rms_norm(hidden_rows, mlp_gain)
        where = places()
        y = jnp.zeros((all_rows, model_width), jnp.bfloat16)
        for start, size in zip(starts, chunk_rows):
            own = slice(start // tp_size, (start + size) // tp_size)
            normed_mlp = lax.all_gather(normed_rows[own], "tp", axis=0, tiled=True)
            gate_pre = jnp.dot(normed_mlp, w_gate, preferred_element_type=jnp.float32)
            up_pre = jnp.dot(normed_mlp, w_up, preferred_element_type=jnp.float32)
            gated = (jax.nn.silu(gate_pre) * up_pre).astype(jnp.bfloat16)
            mlp_part = jnp.dot(gated, w_down, preferred_element_type=jnp.float32).astype(jnp.bfloat16)
            out_rows = reduce_rows(mlp_part, hidden_rows[own], where)
            y_chunk = lax.all_gather(out_rows, "tp", axis=0, tiled=True)
            y = lax.dynamic_update_slice(y, y_chunk, (start, 0))
        return y.reshape(batch_size, seq_len, model_width), k_cache_out, v_cache_out

    cache_spec = P("dp", None, "tp", None)
    return jax.shard_map(layer_shard, mesh=mesh, in_specs=(P("dp", None, None), P("dp"), P(None, "tp"), P(None, "tp"), P(None, "tp"), P("tp", None), P(None, "tp"), P(None, "tp"), P("tp", None), P(), P(), cache_spec, cache_spec), out_specs=(P("dp", None, None), cache_spec, cache_spec), check_vma=False)
```

```python
import jax
import jax.numpy as jnp
from jax import lax
from jax.experimental import pallas as pl
from jax.experimental.pallas import tpu as pltpu
from jax.sharding import PartitionSpec as P


EPS = 1e-5
ROPE_BASE = 10000.0
CHUNK_SEQS = (2, 4, 4, 4, 4, 4, 2)
TILE = 48


def rms_norm(rows, gain):
    rows32 = rows.astype(jnp.float32)
    inv_rms = lax.rsqrt(jnp.mean(rows32 * rows32, axis=-1, keepdims=True) + EPS)
    return (rows32 * inv_rms * gain.astype(jnp.float32)).astype(jnp.bfloat16)


def rotary(vecs):
    seq_len = vecs.shape[1]
    head_dim = vecs.shape[-1]
    half_dim = head_dim // 2
    inv_freq = ROPE_BASE ** (-jnp.arange(0, head_dim, 2).astype(jnp.float32) / head_dim)
    angles = jnp.arange(seq_len).astype(jnp.float32)[:, None] * inv_freq[None, :]
    table_shape = (1, seq_len) + (1,) * (vecs.ndim - 3) + (half_dim,)
    cos_tab = jnp.cos(angles).reshape(table_shape)
    sin_tab = jnp.sin(angles).reshape(table_shape)
    pairs = vecs.reshape(vecs.shape[:-1] + (half_dim, 2))
    even_part = pairs[..., 0]
    odd_part = pairs[..., 1]
    turned = jnp.stack([even_part * cos_tab - odd_part * sin_tab, even_part * sin_tab + odd_part * cos_tab], axis=-1)
    return turned.reshape(vecs.shape).astype(jnp.bfloat16)


def causal_attention(queries, keys, values, seq_lens):
    seq_len = queries.shape[1]
    head_dim = queries.shape[-1]
    scores = jnp.einsum("bqkgh,bskh->bkgqs", queries, keys, preferred_element_type=jnp.float32) * head_dim ** -0.5
    positions = jnp.arange(seq_len)
    allowed = (positions[None, None, :] <= positions[None, :, None]) & (positions[None, None, :] < seq_lens[:, None, None])
    scores = jnp.where(allowed[:, None, None], scores, -jnp.inf)
    probs = jax.nn.softmax(scores, axis=-1).astype(jnp.bfloat16)
    return jnp.einsum("bkgqs,bskh->bqkgh", probs, values, preferred_element_type=jnp.float32).astype(jnp.bfloat16)


def out_kernel(o_ref, w_ref, x_ref, h_ref):
    groups, _, depth = o_ref.shape
    total = jnp.zeros(h_ref.shape, jnp.float32)
    for group in range(groups):
        part = jnp.dot(o_ref[group], w_ref[pl.ds(group * depth, depth), :], preferred_element_type=jnp.float32)
        total = total + part.astype(jnp.bfloat16).astype(jnp.float32)
    h_ref[...] = (x_ref[...].astype(jnp.float32) + total).astype(jnp.bfloat16)


def out_project(o_rows, w_full, x_rows, tile):
    groups, rows, depth = o_rows.shape
    width = w_full.shape[1]
    return pl.pallas_call(
        out_kernel,
        grid=(width // tile,),
        in_specs=[
            pl.BlockSpec((groups, rows, depth), lambda n: (0, 0, 0)),
            pl.BlockSpec((groups * depth, tile), lambda n: (0, n)),
            pl.BlockSpec((rows, tile), lambda n: (0, n)),
        ],
        out_specs=pl.BlockSpec((rows, tile), lambda n: (0, n)),
        out_shape=jax.ShapeDtypeStruct((rows, width), jnp.bfloat16),
        compiler_params=pltpu.CompilerParams(vmem_limit_bytes=56 * 2**20),
        cost_estimate=pl.CostEstimate(flops=2 * rows * groups * depth * width, bytes_accessed=2 * groups * depth * width, transcendentals=0),
        name="out_project",
    )(o_rows, w_full, x_rows)


def wide(ref):
    return ref[0].astype(jnp.float32)


def pieces_kernel(where_ref, far_a, far_b, far_c, far_d, up_a, up_b, down_a, down_b, plus_ref, minus_ref):
    plus_ref[0] = wide(far_a) + wide(far_b)
    plus_ref[1] = wide(up_a) + wide(up_b)
    minus_ref[0] = wide(far_c) + wide(far_d)
    minus_ref[1] = wide(down_a) + wide(down_b)


def runs_kernel(where_ref, up_a, up_b, down_a, down_b, far_low, far_high, low_ref, high_ref):
    low_ref[...] = wide(up_a) + wide(up_b) + far_low[0]
    high_ref[...] = wide(down_a) + wide(down_b) + far_high[0]


def final_kernel(where_ref, low_a, low_b, high_a, high_b, near_low, near_high, run_low, run_high, resid_ref, out_ref):
    half = run_low.shape[1]
    low = wide(low_a) + wide(low_b) + near_low[0] + run_low[...]
    high = wide(high_a) + wide(high_b) + near_high[0] + run_high[...]
    out_ref[:, :half] = (resid_ref[:, :half].astype(jnp.float32) + low).astype(jnp.bfloat16)
    out_ref[:, half:] = (resid_ref[:, half:].astype(jnp.float32) + high).astype(jnp.bfloat16)


def ring_call(kernel, where, operands, specs, out_shapes, out_specs, rows):
    return pl.pallas_call(
        kernel,
        grid_spec=pltpu.PrefetchScalarGridSpec(num_scalar_prefetch=1, grid=(rows // TILE,), in_specs=specs, out_specs=out_specs),
        out_shape=out_shapes,
    )(where, *operands)


def unwritten(shape, dtype):
    return pl.pallas_call(
        lambda out_ref: None,
        out_specs=pl.BlockSpec(memory_space=pl.ANY),
        out_shape=jax.ShapeDtypeStruct(shape, dtype),
        name="unwritten",
    )()


def solution(mesh):
    tp_size = mesh.shape["tp"]
    cores = 2
    chips = tp_size // cores

    def chip_perm(shift):
        return [(chip * cores + core, ((chip + shift) % chips) * cores + core) for chip in range(chips) for core in range(cores)]

    partner_perm = [(index, index ^ 1) for index in range(tp_size)]

    def places():
        chip = lax.shift_right_logical(lax.axis_index("tp"), 1)
        return jnp.stack([(chip + shift) & (chips - 1) for shift in (0, 1, 2, chips - 1)]).astype(jnp.int32)

    def reduce_rows(keep, give, resid_rows, where):
        rows, width = resid_rows.shape
        half = width // 2
        own, up, far, down = range(4)
        low, high = 0, 1

        def move(piece, perm):
            return lax.ppermute(piece, "tp", perm)

        def at(place, side):
            return pl.BlockSpec((1, TILE, half), lambda n, where_ref: (where_ref[place], n, side))

        def part(side):
            return pl.BlockSpec((1, TILE, half), lambda n, where_ref: (side, n, 0))

        flat = pl.BlockSpec((TILE, half), lambda n, where_ref: (n, 0))
        full = pl.BlockSpec((TILE, width), lambda n, where_ref: (n, 0))
        message = jax.ShapeDtypeStruct((2, rows, half), jnp.float32)
        message_spec = pl.BlockSpec((2, TILE, half), lambda n, where_ref: (0, n, 0))
        running = jax.ShapeDtypeStruct((rows, half), jnp.float32)

        got = move(give, partner_perm)
        plus, minus = ring_call(
            pieces_kernel, where, [keep, got] * 4,
            [at(far, low), at(far, low), at(far, high), at(far, high), at(up, high), at(up, high), at(down, low), at(down, low)],
            [message, message], [message_spec, message_spec], rows,
        )
        plus = move(plus, chip_perm(1))
        minus = move(minus, chip_perm(-1))
        run_low, run_high = ring_call(
            runs_kernel, where, [keep, got] * 2 + [plus, minus],
            [at(up, low), at(up, low), at(down, high), at(down, high), part(0), part(0)],
            [running, running], [flat, flat], rows,
        )
        run_low = move(run_low, chip_perm(1))
        run_high = move(run_high, chip_perm(-1))
        return ring_call(
            final_kernel, where, [keep, got] * 2 + [minus, plus, run_low, run_high, resid_rows],
            [at(own, low), at(own, low), at(own, high), at(own, high), part(1), part(1), flat, flat, full],
            jax.ShapeDtypeStruct((rows, width), jnp.bfloat16), full, rows,
        )

    def layer_shard(x, seq_lens, w_query, w_key, w_value, w_out, w_gate, w_up, w_down, attn_gain, mlp_gain, k_cache, v_cache):
        batch_size, seq_len, model_width = x.shape
        head_dim = k_cache.shape[3]
        kv_local = k_cache.shape[2]
        group_size = w_query.shape[1] // (head_dim * kv_local)
        all_rows = batch_size * seq_len
        chunk_rows = [seqs * seq_len for seqs in CHUNK_SEQS]
        starts = [sum(chunk_rows[:chunk]) for chunk in range(len(chunk_rows))]
        tp_index = lax.axis_index("tp")
        w_out_full = lax.all_gather(w_out, "tp", axis=0, tiled=True)
        normed = rms_norm(x, attn_gain)
        queries = rotary(jnp.einsum("bsd,dk->bsk", normed, w_query, preferred_element_type=jnp.float32).reshape(batch_size, seq_len, kv_local, group_size, head_dim))
        keys = rotary(jnp.einsum("bsd,dk->bsk", normed, w_key, preferred_element_type=jnp.float32).reshape(batch_size, seq_len, kv_local, head_dim))
        values = jnp.einsum("bsd,dk->bsk", normed, w_value, preferred_element_type=jnp.float32).astype(jnp.bfloat16).reshape(batch_size, seq_len, kv_local, head_dim)
        valid = (jnp.arange(seq_len)[None, :] < seq_lens[:, None])[:, :, None, None]
        keys = jnp.where(valid, keys, jnp.zeros_like(keys))
        values = jnp.where(valid, values, jnp.zeros_like(values))
        k_cache_out = lax.dynamic_update_slice(k_cache, keys, (0, 0, 0, 0))
        v_cache_out = lax.dynamic_update_slice(v_cache, values, (0, 0, 0, 0))
        attn_rows = causal_attention(queries, keys, values, seq_lens).reshape(all_rows, -1)

        def by_owner(array):
            pieces = [array[start:start + size].reshape(tp_size, size // tp_size, array.shape[1]) for start, size in zip(starts, chunk_rows)]
            return jnp.concatenate(pieces, axis=1)

        o_rows = lax.all_to_all(by_owner(attn_rows), "tp", 0, 0, tiled=True)
        x_rows = jnp.concatenate([lax.dynamic_slice_in_dim(x.reshape(all_rows, model_width), start + tp_index * (size // tp_size), size // tp_size, axis=0) for start, size in zip(starts, chunk_rows)], axis=0)
        first = chunk_rows[0] // tp_size
        fence = lax.optimization_barrier
        hidden_first = out_project(o_rows[:, :first], w_out_full, x_rows[:first], 512)
        normed_first, o_rest = fence((rms_norm(hidden_first, mlp_gain), o_rows[:, first:]))
        hidden_rest = out_project(o_rest, w_out_full, x_rows[first:], 512)
        hidden = [hidden_first, hidden_rest]
        normed_parts = [normed_first, rms_norm(hidden_rest, mlp_gain)]
        keep = hidden_first
        where = places()
        core = lax.axis_index("tp") & 1
        y = unwritten((all_rows, model_width), jnp.bfloat16)
        for chunk, (start, size) in enumerate(zip(starts, chunk_rows)):
            rows = size // tp_size
            begin = start // tp_size - (first if chunk else 0)
            own = slice(begin, begin + rows)
            normed_mlp = lax.all_gather(normed_parts[min(chunk, 1)][own], "tp", axis=0, tiled=True)
            if chunk:
                normed_mlp, keep = fence((normed_mlp, keep))
            gate_pre = jnp.dot(normed_mlp, w_gate, preferred_element_type=jnp.float32)
            up_pre = jnp.dot(normed_mlp, w_up, preferred_element_type=jnp.float32)
            gated = (jax.nn.silu(gate_pre) * up_pre).astype(jnp.bfloat16)

            def down(which, gated):
                blocks = gated.reshape(chips, cores, rows, gated.shape[1])
                picked = lax.dynamic_slice(blocks, (0, which, 0, 0), (chips, 1, rows, gated.shape[1]), allow_negative_indices=False)
                partial = jnp.dot(picked.reshape(chips * rows, gated.shape[1]), w_down, preferred_element_type=jnp.float32)
                return partial.astype(jnp.bfloat16).reshape(chips, rows, model_width)

            gated, core = fence((gated, core))
            give = down(1 - core, gated)
            gated, give, core = fence((gated, give, core))
            keep = down(core, gated)
            out_rows = reduce_rows(keep, give, hidden[min(chunk, 1)][own], where)
            y_chunk = lax.all_gather(out_rows, "tp", axis=0, tiled=True)
            y = lax.dynamic_update_slice(y, y_chunk, (start, 0))
        return y.reshape(batch_size, seq_len, model_width), k_cache_out, v_cache_out

    cache_spec = P("dp", None, "tp", None)
    return jax.shard_map(layer_shard, mesh=mesh, in_specs=(P("dp", None, None), P("dp"), P(None, "tp"), P(None, "tp"), P(None, "tp"), P("tp", None), P(None, "tp"), P(None, "tp"), P("tp", None), P(), P(), cache_spec, cache_spec), out_specs=(P("dp", None, None), cache_spec, cache_spec), check_vma=False)
```

```python
import jax
import jax.numpy as jnp
from jax import lax
from jax.experimental import pallas as pl
from jax.experimental.pallas import tpu as pltpu
from jax.sharding import PartitionSpec as P


EPS = 1e-5
ROPE_BASE = 10000.0
CHUNK_PARTS = (3, 4, 4, 4, 3)
TILE = 32


def rms_norm(rows, gain):
    rows32 = rows.astype(jnp.float32)
    inv_rms = lax.rsqrt(jnp.mean(rows32 * rows32, axis=-1, keepdims=True) + EPS)
    return (rows32 * inv_rms * gain.astype(jnp.float32)).astype(jnp.bfloat16)


def rotary(vecs):
    seq_len = vecs.shape[1]
    head_dim = vecs.shape[-1]
    half_dim = head_dim // 2
    inv_freq = ROPE_BASE ** (-jnp.arange(0, head_dim, 2).astype(jnp.float32) / head_dim)
    angles = jnp.arange(seq_len).astype(jnp.float32)[:, None] * inv_freq[None, :]
    table_shape = (1, seq_len) + (1,) * (vecs.ndim - 3) + (half_dim,)
    cos_tab = jnp.cos(angles).reshape(table_shape)
    sin_tab = jnp.sin(angles).reshape(table_shape)
    pairs = vecs.reshape(vecs.shape[:-1] + (half_dim, 2))
    even_part = pairs[..., 0]
    odd_part = pairs[..., 1]
    turned = jnp.stack([even_part * cos_tab - odd_part * sin_tab, even_part * sin_tab + odd_part * cos_tab], axis=-1)
    return turned.reshape(vecs.shape).astype(jnp.bfloat16)


def causal_attention(queries, keys, values, seq_lens):
    seq_len = queries.shape[1]
    head_dim = queries.shape[-1]
    scores = jnp.einsum("bqkgh,bskh->bkgqs", queries, keys, preferred_element_type=jnp.float32) * head_dim ** -0.5
    positions = jnp.arange(seq_len)
    allowed = (positions[None, None, :] <= positions[None, :, None]) & (positions[None, None, :] < seq_lens[:, None, None])
    scores = jnp.where(allowed[:, None, None], scores, -jnp.inf)
    probs = jax.nn.softmax(scores, axis=-1).astype(jnp.bfloat16)
    return jnp.einsum("bkgqs,bskh->bqkgh", probs, values, preferred_element_type=jnp.float32).astype(jnp.bfloat16)


def out_kernel(o_ref, w_ref, x_ref, h_ref):
    groups, _, depth = o_ref.shape
    total = jnp.zeros(h_ref.shape, jnp.float32)
    for group in range(groups):
        part = jnp.dot(o_ref[group], w_ref[pl.ds(group * depth, depth), :], preferred_element_type=jnp.float32)
        total = total + part.astype(jnp.bfloat16).astype(jnp.float32)
    h_ref[...] = (x_ref[...].astype(jnp.float32) + total).astype(jnp.bfloat16)


def out_project(o_rows, w_full, x_rows, tile):
    groups, rows, depth = o_rows.shape
    width = w_full.shape[1]
    return pl.pallas_call(
        out_kernel,
        grid=(width // tile,),
        in_specs=[
            pl.BlockSpec((groups, rows, depth), lambda n: (0, 0, 0)),
            pl.BlockSpec((groups * depth, tile), lambda n: (0, n)),
            pl.BlockSpec((rows, tile), lambda n: (0, n)),
        ],
        out_specs=pl.BlockSpec((rows, tile), lambda n: (0, n)),
        out_shape=jax.ShapeDtypeStruct((rows, width), jnp.bfloat16),
        compiler_params=pltpu.CompilerParams(vmem_limit_bytes=56 * 2**20),
        cost_estimate=pl.CostEstimate(flops=2 * rows * groups * depth * width, bytes_accessed=2 * groups * depth * width, transcendentals=0),
        name="out_project",
    )(o_rows, w_full, x_rows)


def wide(ref):
    return ref[...].reshape(ref.shape[-2:]).astype(jnp.float32)


def pieces_kernel(where_ref, far_a, far_b, far_c, far_d, up_a, up_b, down_a, down_b, plus_ref, minus_ref):
    plus_ref[0] = wide(far_a) + wide(far_b)
    plus_ref[1] = wide(up_a) + wide(up_b)
    minus_ref[0] = wide(far_c) + wide(far_d)
    minus_ref[1] = wide(down_a) + wide(down_b)


def runs_kernel(where_ref, up_a, up_b, down_a, down_b, far_low, far_high, low_ref, high_ref):
    low_ref[...] = wide(up_a) + wide(up_b) + far_low[0]
    high_ref[...] = wide(down_a) + wide(down_b) + far_high[0]


def final_kernel(where_ref, low_a, low_b, high_a, high_b, near_low, near_high, run_low, run_high, resid_ref, out_ref):
    half = run_low.shape[1]
    low = wide(low_a) + wide(low_b) + near_low[0] + run_low[...]
    high = wide(high_a) + wide(high_b) + near_high[0] + run_high[...]
    out_ref[:, :half] = (resid_ref[:, :half].astype(jnp.float32) + low).astype(jnp.bfloat16)
    out_ref[:, half:] = (resid_ref[:, half:].astype(jnp.float32) + high).astype(jnp.bfloat16)


def ring_call(kernel, where, operands, specs, out_shapes, out_specs, rows):
    return pl.pallas_call(
        kernel,
        grid_spec=pltpu.PrefetchScalarGridSpec(num_scalar_prefetch=1, grid=(rows // TILE,), in_specs=specs, out_specs=out_specs),
        out_shape=out_shapes,
    )(where, *operands)


def unwritten(shape, dtype):
    return pl.pallas_call(
        lambda out_ref: None,
        out_specs=pl.BlockSpec(memory_space=pl.ANY),
        out_shape=jax.ShapeDtypeStruct(shape, dtype),
        name="unwritten",
    )()


def solution(mesh):
    tp_size = mesh.shape["tp"]
    cores = 2
    chips = tp_size // cores

    def chip_perm(shift):
        return [(chip * cores + core, ((chip + shift) % chips) * cores + core) for chip in range(chips) for core in range(cores)]

    partner_perm = [(index, index ^ 1) for index in range(tp_size)]

    def places():
        index = lax.axis_index("tp")
        chip = lax.shift_right_logical(index, 1)
        return jnp.stack([(chip + shift) & (chips - 1) for shift in (0, 1, 2, chips - 1)] + [index & 1]).astype(jnp.int32)

    def reduce_rows(partial, give, resid_rows, where):
        rows, width = resid_rows.shape
        half = width // 2
        own, up, far, down = range(4)
        low, high = 0, 1

        def move(piece, perm):
            return lax.ppermute(piece, "tp", perm)

        def at(place, side):
            mine = pl.BlockSpec((1, 1, TILE, half), lambda n, where_ref: (where_ref[place], where_ref[4], n, side))
            theirs = pl.BlockSpec((1, TILE, half), lambda n, where_ref: (where_ref[place], n, side))
            return [mine, theirs]

        def part(side):
            return pl.BlockSpec((1, TILE, half), lambda n, where_ref: (side, n, 0))

        flat = pl.BlockSpec((TILE, half), lambda n, where_ref: (n, 0))
        full = pl.BlockSpec((TILE, width), lambda n, where_ref: (n, 0))
        message = jax.ShapeDtypeStruct((2, rows, half), jnp.float32)
        message_spec = pl.BlockSpec((2, TILE, half), lambda n, where_ref: (0, n, 0))
        running = jax.ShapeDtypeStruct((rows, half), jnp.float32)

        got = move(give, partner_perm)
        plus, minus = ring_call(
            pieces_kernel, where, [partial, got] * 4,
            at(far, low) + at(far, high) + at(up, high) + at(down, low),
            [message, message], [message_spec, message_spec], rows,
        )
        plus = move(plus, chip_perm(1))
        minus = move(minus, chip_perm(-1))
        run_low, run_high = ring_call(
            runs_kernel, where, [partial, got] * 2 + [plus, minus],
            at(up, low) + at(down, high) + [part(0), part(0)],
            [running, running], [flat, flat], rows,
        )
        run_low = move(run_low, chip_perm(1))
        run_high = move(run_high, chip_perm(-1))
        return ring_call(
            final_kernel, where, [partial, got] * 2 + [minus, plus, run_low, run_high, resid_rows],
            at(own, low) + at(own, high) + [part(1), part(1), flat, flat, full],
            jax.ShapeDtypeStruct((rows, width), jnp.bfloat16), full, rows,
        )

    def layer_shard(x, seq_lens, w_query, w_key, w_value, w_out, w_gate, w_up, w_down, attn_gain, mlp_gain, k_cache, v_cache):
        batch_size, seq_len, model_width = x.shape
        head_dim = k_cache.shape[3]
        kv_local = k_cache.shape[2]
        group_size = w_query.shape[1] // (head_dim * kv_local)
        all_rows = batch_size * seq_len
        owned = all_rows // tp_size
        chunk_rows = [owned * share // sum(CHUNK_PARTS) for share in CHUNK_PARTS]
        starts = [sum(chunk_rows[:chunk]) for chunk in range(len(chunk_rows))]
        tp_index = lax.axis_index("tp")
        w_out_full = lax.all_gather(w_out, "tp", axis=0, tiled=True)
        normed = rms_norm(x, attn_gain)
        queries = rotary(jnp.einsum("bsd,dk->bsk", normed, w_query, preferred_element_type=jnp.float32).reshape(batch_size, seq_len, kv_local, group_size, head_dim))
        keys = rotary(jnp.einsum("bsd,dk->bsk", normed, w_key, preferred_element_type=jnp.float32).reshape(batch_size, seq_len, kv_local, head_dim))
        values = jnp.einsum("bsd,dk->bsk", normed, w_value, preferred_element_type=jnp.float32).astype(jnp.bfloat16).reshape(batch_size, seq_len, kv_local, head_dim)
        valid = (jnp.arange(seq_len)[None, :] < seq_lens[:, None])[:, :, None, None]
        keys = jnp.where(valid, keys, jnp.zeros_like(keys))
        values = jnp.where(valid, values, jnp.zeros_like(values))
        k_cache_out = lax.dynamic_update_slice(k_cache, keys, (0, 0, 0, 0))
        v_cache_out = lax.dynamic_update_slice(v_cache, values, (0, 0, 0, 0))
        attn_rows = causal_attention(queries, keys, values, seq_lens).reshape(tp_size, owned, -1)
        o_rows = lax.all_to_all(attn_rows, "tp", 0, 0, tiled=True)
        x_rows = lax.dynamic_slice_in_dim(x.reshape(all_rows, model_width), tp_index * owned, owned, axis=0)
        first = chunk_rows[0]
        fence = lax.optimization_barrier
        hidden_first = out_project(o_rows[:, :first], w_out_full, x_rows[:first], 512)
        normed_first, o_rest = fence((rms_norm(hidden_first, mlp_gain), o_rows[:, first:]))
        hidden_rest = out_project(o_rest, w_out_full, x_rows[first:], 512)
        hidden = [hidden_first, hidden_rest]
        normed_parts = [normed_first, rms_norm(hidden_rest, mlp_gain)]
        partial = hidden_first
        where = places()
        core = tp_index & 1
        y = unwritten((tp_size, owned, model_width), jnp.bfloat16)
        for chunk, (start, rows) in enumerate(zip(starts, chunk_rows)):
            begin = start - first if chunk else 0
            own = slice(begin, begin + rows)
            normed_mlp = lax.all_gather(normed_parts[min(chunk, 1)][own], "tp", axis=0, tiled=True)
            if chunk:
                normed_mlp, partial = fence((normed_mlp, partial))
            gate_pre = jnp.dot(normed_mlp, w_gate, preferred_element_type=jnp.float32)
            up_pre = jnp.dot(normed_mlp, w_up, preferred_element_type=jnp.float32)
            gated = (jax.nn.silu(gate_pre) * up_pre).astype(jnp.bfloat16)
            partial = jnp.dot(gated, w_down, preferred_element_type=jnp.float32).astype(jnp.bfloat16)
            partial, core = fence((partial, core))
            blocks = partial.reshape(chips, cores, rows, model_width)
            give = lax.dynamic_slice(blocks, (0, 1 - core, 0, 0), (chips, 1, rows, model_width), allow_negative_indices=False)
            give, core = fence((give.reshape(chips, rows, model_width), core))
            out_rows = reduce_rows(blocks, give, hidden[min(chunk, 1)][own], where)
            y_chunk = lax.all_gather(out_rows, "tp", axis=0)
            y = lax.dynamic_update_slice(y, y_chunk, (0, start, 0))
        return y.reshape(batch_size, seq_len, model_width), k_cache_out, v_cache_out

    cache_spec = P("dp", None, "tp", None)
    return jax.shard_map(layer_shard, mesh=mesh, in_specs=(P("dp", None, None), P("dp"), P(None, "tp"), P(None, "tp"), P(None, "tp"), P("tp", None), P(None, "tp"), P(None, "tp"), P("tp", None), P(), P(), cache_spec, cache_spec), out_specs=(P("dp", None, None), cache_spec, cache_spec), check_vma=False)
```

```python
import jax
import jax.numpy as jnp
from jax import lax
from jax.experimental import pallas as pl
from jax.experimental.pallas import tpu as pltpu
from jax.sharding import PartitionSpec as P


EPS = 1e-5
ROPE_BASE = 10000.0
CHUNK_PARTS = (8, 7, 6, 6, 6, 3)
TILES = (32, 16)


def rms_norm(rows, gain):
    rows32 = rows.astype(jnp.float32)
    inv_rms = lax.rsqrt(jnp.mean(rows32 * rows32, axis=-1, keepdims=True) + EPS)
    return (rows32 * inv_rms * gain.astype(jnp.float32)).astype(jnp.bfloat16)


def rotary(vecs):
    seq_len = vecs.shape[1]
    head_dim = vecs.shape[-1]
    half_dim = head_dim // 2
    inv_freq = ROPE_BASE ** (-jnp.arange(0, head_dim, 2).astype(jnp.float32) / head_dim)
    angles = jnp.arange(seq_len).astype(jnp.float32)[:, None] * inv_freq[None, :]
    table_shape = (1, seq_len) + (1,) * (vecs.ndim - 3) + (half_dim,)
    cos_tab = jnp.cos(angles).reshape(table_shape)
    sin_tab = jnp.sin(angles).reshape(table_shape)
    pairs = vecs.reshape(vecs.shape[:-1] + (half_dim, 2))
    even_part = pairs[..., 0]
    odd_part = pairs[..., 1]
    turned = jnp.stack([even_part * cos_tab - odd_part * sin_tab, even_part * sin_tab + odd_part * cos_tab], axis=-1)
    return turned.reshape(vecs.shape).astype(jnp.bfloat16)


def causal_attention(queries, keys, values, seq_lens):
    seq_len = queries.shape[1]
    head_dim = queries.shape[-1]
    scores = jnp.einsum("bqkgh,bskh->bkgqs", queries, keys, preferred_element_type=jnp.float32) * head_dim ** -0.5
    positions = jnp.arange(seq_len)
    allowed = (positions[None, None, :] <= positions[None, :, None]) & (positions[None, None, :] < seq_lens[:, None, None])
    scores = jnp.where(allowed[:, None, None], scores, -jnp.inf)
    probs = jax.nn.softmax(scores, axis=-1).astype(jnp.bfloat16)
    return jnp.einsum("bkgqs,bskh->bqkgh", probs, values, preferred_element_type=jnp.float32).astype(jnp.bfloat16)


def out_kernel(o_ref, w_ref, x_ref, h_ref):
    groups, _, depth = o_ref.shape
    total = jnp.zeros(h_ref.shape, jnp.float32)
    for group in range(groups):
        part = jnp.dot(o_ref[group], w_ref[pl.ds(group * depth, depth), :], preferred_element_type=jnp.float32)
        total = total + part.astype(jnp.bfloat16).astype(jnp.float32)
    h_ref[...] = (x_ref[...].astype(jnp.float32) + total).astype(jnp.bfloat16)


def out_project(o_rows, w_full, x_rows, tile):
    groups, rows, depth = o_rows.shape
    width = w_full.shape[1]
    return pl.pallas_call(
        out_kernel,
        grid=(width // tile,),
        in_specs=[
            pl.BlockSpec((groups, rows, depth), lambda n: (0, 0, 0)),
            pl.BlockSpec((groups * depth, tile), lambda n: (0, n)),
            pl.BlockSpec((rows, tile), lambda n: (0, n)),
        ],
        out_specs=pl.BlockSpec((rows, tile), lambda n: (0, n)),
        out_shape=jax.ShapeDtypeStruct((rows, width), jnp.bfloat16),
        compiler_params=pltpu.CompilerParams(vmem_limit_bytes=56 * 2**20),
        cost_estimate=pl.CostEstimate(flops=2 * rows * groups * depth * width, bytes_accessed=2 * groups * depth * width, transcendentals=0),
        name="out_project",
    )(o_rows, w_full, x_rows)


def row_tile(rows):
    return next(tile for tile in TILES if rows % tile == 0)


def wide(ref):
    return ref[...].reshape(ref.shape[-2:]).astype(jnp.float32)


def pieces_kernel(where_ref, far_a, far_b, far_c, far_d, up_a, up_b, down_a, down_b, plus_ref, minus_ref):
    plus_ref[0] = wide(far_a) + wide(far_b)
    plus_ref[1] = wide(up_a) + wide(up_b)
    minus_ref[0] = wide(far_c) + wide(far_d)
    minus_ref[1] = wide(down_a) + wide(down_b)


def runs_kernel(where_ref, up_a, up_b, down_a, down_b, far_low, far_high, low_ref, high_ref):
    low_ref[...] = wide(up_a) + wide(up_b) + far_low[0]
    high_ref[...] = wide(down_a) + wide(down_b) + far_high[0]


def final_kernel(where_ref, low_a, low_b, high_a, high_b, near_low, near_high, run_low, run_high, resid_ref, out_ref):
    half = run_low.shape[1]
    low = wide(low_a) + wide(low_b) + near_low[0] + run_low[...]
    high = wide(high_a) + wide(high_b) + near_high[0] + run_high[...]
    out_ref[:, :half] = (resid_ref[:, :half].astype(jnp.float32) + low).astype(jnp.bfloat16)
    out_ref[:, half:] = (resid_ref[:, half:].astype(jnp.float32) + high).astype(jnp.bfloat16)


def ring_call(kernel, where, operands, specs, out_shapes, out_specs, rows):
    return pl.pallas_call(
        kernel,
        grid_spec=pltpu.PrefetchScalarGridSpec(num_scalar_prefetch=1, grid=(rows // row_tile(rows),), in_specs=specs, out_specs=out_specs),
        out_shape=out_shapes,
    )(where, *operands)


def unwritten(shape, dtype):
    return pl.pallas_call(
        lambda out_ref: None,
        out_specs=pl.BlockSpec(memory_space=pl.ANY),
        out_shape=jax.ShapeDtypeStruct(shape, dtype),
        name="unwritten",
    )()


def solution(mesh):
    tp_size = mesh.shape["tp"]
    cores = 2
    chips = tp_size // cores

    def chip_perm(shift):
        return [(chip * cores + core, ((chip + shift) % chips) * cores + core) for chip in range(chips) for core in range(cores)]

    partner_perm = [(index, index ^ 1) for index in range(tp_size)]

    def places():
        index = lax.axis_index("tp")
        chip = lax.shift_right_logical(index, 1)
        return jnp.stack([(chip + shift) & (chips - 1) for shift in (0, 1, 2, chips - 1)] + [index & 1]).astype(jnp.int32)

    def reduce_rows(partial, give, resid_rows, where):
        rows, width = resid_rows.shape
        half = width // 2
        tile = row_tile(rows)
        own, up, far, down = range(4)
        low, high = 0, 1

        def move(piece, perm):
            return lax.ppermute(piece, "tp", perm)

        def at(place, side):
            mine = pl.BlockSpec((1, 1, tile, half), lambda n, where_ref: (where_ref[place], where_ref[4], n, side))
            theirs = pl.BlockSpec((1, tile, half), lambda n, where_ref: (where_ref[place], n, side))
            return [mine, theirs]

        def part(side):
            return pl.BlockSpec((1, tile, half), lambda n, where_ref: (side, n, 0))

        flat = pl.BlockSpec((tile, half), lambda n, where_ref: (n, 0))
        full = pl.BlockSpec((tile, width), lambda n, where_ref: (n, 0))
        message = jax.ShapeDtypeStruct((2, rows, half), jnp.float32)
        message_spec = pl.BlockSpec((2, tile, half), lambda n, where_ref: (0, n, 0))
        running = jax.ShapeDtypeStruct((rows, half), jnp.float32)

        got = move(give, partner_perm)
        plus, minus = ring_call(
            pieces_kernel, where, [partial, got] * 4,
            at(far, low) + at(far, high) + at(up, high) + at(down, low),
            [message, message], [message_spec, message_spec], rows,
        )
        plus = move(plus, chip_perm(1))
        minus = move(minus, chip_perm(-1))
        run_low, run_high = ring_call(
            runs_kernel, where, [partial, got] * 2 + [plus, minus],
            at(up, low) + at(down, high) + [part(0), part(0)],
            [running, running], [flat, flat], rows,
        )
        run_low = move(run_low, chip_perm(1))
        run_high = move(run_high, chip_perm(-1))
        return ring_call(
            final_kernel, where, [partial, got] * 2 + [minus, plus, run_low, run_high, resid_rows],
            at(own, low) + at(own, high) + [part(1), part(1), flat, flat, full],
            jax.ShapeDtypeStruct((rows, width), jnp.bfloat16), full, rows,
        )

    def layer_shard(x, seq_lens, w_query, w_key, w_value, w_out, w_gate, w_up, w_down, attn_gain, mlp_gain, k_cache, v_cache):
        batch_size, seq_len, model_width = x.shape
        head_dim = k_cache.shape[3]
        kv_local = k_cache.shape[2]
        group_size = w_query.shape[1] // (head_dim * kv_local)
        all_rows = batch_size * seq_len
        owned = all_rows // tp_size
        chunk_rows = [owned * share // sum(CHUNK_PARTS) for share in CHUNK_PARTS]
        starts = [sum(chunk_rows[:chunk]) for chunk in range(len(chunk_rows))]
        tp_index = lax.axis_index("tp")
        w_out_full = lax.all_gather(w_out, "tp", axis=0, tiled=True)
        normed = rms_norm(x, attn_gain)
        queries = rotary(jnp.einsum("bsd,dk->bsk", normed, w_query, preferred_element_type=jnp.float32).reshape(batch_size, seq_len, kv_local, group_size, head_dim))
        keys = rotary(jnp.einsum("bsd,dk->bsk", normed, w_key, preferred_element_type=jnp.float32).reshape(batch_size, seq_len, kv_local, head_dim))
        values = jnp.einsum("bsd,dk->bsk", normed, w_value, preferred_element_type=jnp.float32).astype(jnp.bfloat16).reshape(batch_size, seq_len, kv_local, head_dim)
        valid = (jnp.arange(seq_len)[None, :] < seq_lens[:, None])[:, :, None, None]
        keys = jnp.where(valid, keys, jnp.zeros_like(keys))
        values = jnp.where(valid, values, jnp.zeros_like(values))
        k_cache_out = lax.dynamic_update_slice(k_cache, keys, (0, 0, 0, 0))
        v_cache_out = lax.dynamic_update_slice(v_cache, values, (0, 0, 0, 0))
        attn_rows = causal_attention(queries, keys, values, seq_lens).reshape(tp_size, owned, -1)
        o_rows = lax.all_to_all(attn_rows, "tp", 0, 0, tiled=True)
        x_rows = lax.dynamic_slice_in_dim(x.reshape(all_rows, model_width), tp_index * owned, owned, axis=0)
        first = chunk_rows[0]
        fence = lax.optimization_barrier
        hidden_first = out_project(o_rows[:, :first], w_out_full, x_rows[:first], 512)
        normed_first, o_rest = fence((rms_norm(hidden_first, mlp_gain), o_rows[:, first:]))
        hidden_rest = out_project(o_rest, w_out_full, x_rows[first:], 512)
        hidden = [hidden_first, hidden_rest]
        normed_parts = [normed_first, rms_norm(hidden_rest, mlp_gain)]
        partial = hidden_first
        where = places()
        core = tp_index & 1
        y = unwritten((tp_size, owned, model_width), jnp.bfloat16)
        for chunk, (start, rows) in enumerate(zip(starts, chunk_rows)):
            begin = start - first if chunk else 0
            own = slice(begin, begin + rows)
            normed_mlp = lax.all_gather(normed_parts[min(chunk, 1)][own], "tp", axis=0, tiled=True)
            if chunk:
                normed_mlp, partial = fence((normed_mlp, partial))
            gate_pre = jnp.dot(normed_mlp, w_gate, preferred_element_type=jnp.float32)
            up_pre = jnp.dot(normed_mlp, w_up, preferred_element_type=jnp.float32)
            gated = (jax.nn.silu(gate_pre) * up_pre).astype(jnp.bfloat16)
            partial = jnp.dot(gated, w_down, preferred_element_type=jnp.float32).astype(jnp.bfloat16)
            partial, core = fence((partial, core))
            blocks = partial.reshape(chips, cores, rows, model_width)
            give = lax.dynamic_slice(blocks, (0, 1 - core, 0, 0), (chips, 1, rows, model_width), allow_negative_indices=False)
            give, core = fence((give.reshape(chips, rows, model_width), core))
            out_rows = reduce_rows(blocks, give, hidden[min(chunk, 1)][own], where)
            y_chunk = lax.all_gather(out_rows, "tp", axis=0)
            y = lax.dynamic_update_slice(y, y_chunk, (0, start, 0))
        return y.reshape(batch_size, seq_len, model_width), k_cache_out, v_cache_out

    cache_spec = P("dp", None, "tp", None)
    return jax.shard_map(layer_shard, mesh=mesh, in_specs=(P("dp", None, None), P("dp"), P(None, "tp"), P(None, "tp"), P(None, "tp"), P("tp", None), P(None, "tp"), P(None, "tp"), P("tp", None), P(), P(), cache_spec, cache_spec), out_specs=(P("dp", None, None), cache_spec, cache_spec), check_vma=False)
```
